256 devices in a mesh: head: 8 (over x_hi, y), inner: 2 (over x_lo), outer: 16 (over z, core).
Axes of the slice: x: 4 (x_hi: 2, x_lo: 2; x = x_hi * 2 + x_lo), y: 4, z: 8, core: 2. Of those that a mesh axis runs over, the one named last changes fastest.
Arguments:
- query_nope: bfloat16 [4096, 8192], P(('inner', 'outer'), 'head'), may hold values from -6 to 6
- query_rope: bfloat16 [4096, 4096], P(('inner', 'outer'), 'head'), may hold values from -256 to 256
- latent: bfloat16 [4096, 512], P(('inner', 'outer')), may hold values from -6 to 6
- key_rope: bfloat16 [4096, 64], P(('inner', 'outer')), may hold values from -4 to 4
- key_up: bfloat16 [512, 8192], P(None, 'head'), may hold values from -0.25 to 0.25
- value_up: bfloat16 [512, 8192], P(None, 'head'), may hold values from -0.25 to 0.25
- latent_out: bfloat16 [4096, 32768], P(('inner', 'outer'), 'head'), may hold values from -3 to 3
- out_grad: bfloat16 [4096, 8192], P(('inner', 'outer'), 'head'), may hold values from -6 to 6
- logsum: float32 [4096, 64], P(('inner', 'outer'), 'head'), may hold values from 0 to 5000
- block_order: int32 [64], replicated, may hold values from 0 to 63, as said below
Outputs:
- d_query_nope: bfloat16 [4096, 8192], P(('inner', 'outer'), 'head')
- d_query_rope: bfloat16 [4096, 4096], P(('inner', 'outer'), 'head')
- d_latent: bfloat16 [4096, 512], P(('inner', 'outer'))
- d_key_rope: bfloat16 [4096, 64], P(('inner', 'outer'))
- d_key_up: float32 [512, 8192], P(('inner', 'outer'), 'head')
- d_value_up: float32 [512, 8192], P(('inner', 'outer'), 'head')
The draws below stay inside these ranges and needn't reach their ends.
Inputs may be any that keep to these rules, and one draw needn't show every extreme that they name: `block_order`: stored blocks 2 r and 2 r + 1 hold sequence blocks c and 63 - c for some c, in either order; every sequence block is held once.
All inputs are finite; a program needn't handle non-finite values.
Results may differ from the reference program's by a relative error of at most 0.0085.
The reference program's roundings to bfloat16 on the way count: a program that leaves them out, or rounds other values in their place, can miss the bound.
Values may be sent and summed in bfloat16 or wider, within the bound.
No kernel may reach another device: no remote copies, remote signals or barrier semaphores. Data moves between devices by JAX's collectives and lax.ppermute only.
A program may use at most 128 MiB of HBM per device.

```python
import jax
import jax.numpy as jnp
from jax import lax

HEADS = 64
LATENT = 512
ROPE_DIM = 64
NOPE_DIM = 128
VALUE_DIM = 128
BLOCK_ROWS = 64
SEQUENCE = 4096
BLOCKS = 64


def rope_helper(key):
    baseline = jnp.clip(jax.random.normal(jax.random.fold_in(key, 11), (SEQUENCE, ROPE_DIM), jnp.float32), -4.0, 4.0)
    return baseline


def draw_key_rope(key, part):
    baseline = rope_helper(key)
    return baseline.astype(jnp.bfloat16)


def draw_query_rope(key, part):
    values = jnp.clip(jax.random.normal(jax.random.fold_in(key, 14), (SEQUENCE, HEADS * ROPE_DIM), jnp.float32), -4.0, 4.0)
    return values.astype(jnp.bfloat16)


def draw_block_order(key, part):
    pairs = BLOCKS // 2
    smaller = jax.random.permutation(jax.random.fold_in(key, 21), pairs).astype(jnp.int32)
    flipped = jax.random.randint(jax.random.fold_in(key, 22), (pairs,), 0, 2)
    larger = BLOCKS - 1 - smaller
    first_held = jnp.where(flipped == 1, larger, smaller)
    second_held = jnp.where(flipped == 1, smaller, larger)
    return jnp.stack([first_held, second_held], axis=1).reshape(BLOCKS).astype(jnp.int32)


def draw_logsum(key, part):
    order = draw_block_order(key, part)
    indices = jnp.arange(SEQUENCE, dtype=jnp.int32)
    places = (order[indices // BLOCK_ROWS] * BLOCK_ROWS + indices % BLOCK_ROWS).astype(jnp.float32)
    counted = jnp.log(places + 1.0) + 1.5
    noise = jax.random.uniform(jax.random.fold_in(key, 31), (SEQUENCE, HEADS), jnp.float32, 0.0, 1.0)
    values = counted[:, None] + noise
    return jnp.clip(values, 0.0, 5000.0).astype(jnp.float32)


def steps_of(own_key, shape, split, low, largest):
    def one(position, blocks):
        heights = jax.random.uniform(jax.random.fold_in(jax.random.fold_in(own_key, 6), position), (blocks,), jnp.float32, low / len(split), largest / len(split))
        return jnp.repeat(jnp.exp(heights), shape[position] // blocks).reshape((-1,) + (1,) * (len(shape) - position - 1))

    gain = one(*split[0])
    for cut in split[1:]:
        gain = gain * one(*cut)
    return gain


def centred(stream_key, dims, deviation, limit, split=(), kind=jnp.bfloat16):
    entries = deviation * jax.random.normal(stream_key, dims, jnp.float32)
    if split:
        entries = entries * steps_of(stream_key, dims, split, -0.22, 0.18)
    return jnp.clip(entries, -limit, limit).astype(kind)


def setup_inputs(seed: int = 0) -> dict:
    arg_keys = jax.random.split(jax.random.key(seed), 11)
    return {
        "query_nope": centred(arg_keys[0], (SEQUENCE, HEADS * NOPE_DIM), 1.0, 6.0, ((0, 32), (1, 8))),
        "query_rope": draw_query_rope(jax.random.fold_in(arg_keys[10], 71), 0),
        "latent": centred(arg_keys[2], (SEQUENCE, LATENT), 1.0, 6.0, ((0, 32),)),
        "key_rope": draw_key_rope(jax.random.fold_in(arg_keys[10], 71), 0),
        "key_up": centred(arg_keys[4], (LATENT, HEADS * NOPE_DIM), LATENT ** -0.5, 0.25, ((1, 8),)),
        "value_up": centred(arg_keys[5], (LATENT, HEADS * VALUE_DIM), LATENT ** -0.5, 0.25, ((1, 8),)),
        "latent_out": centred(arg_keys[6], (SEQUENCE, HEADS * LATENT), 0.5, 3.0, ((0, 32), (1, 8))),
        "out_grad": centred(arg_keys[7], (SEQUENCE, HEADS * VALUE_DIM), 1.0, 6.0, ((0, 32), (1, 8))),
        "logsum": draw_logsum(jax.random.fold_in(arg_keys[10], 71), 0),
        "block_order": draw_block_order(jax.random.fold_in(arg_keys[10], 71), 0),
    }


def stored_positions(block_order):
    indices = jnp.arange(SEQUENCE, dtype=jnp.int32)
    return block_order[indices // BLOCK_ROWS].astype(jnp.int32) * BLOCK_ROWS + indices % BLOCK_ROWS


def by_head(matrix, width):
    return matrix.reshape(matrix.shape[0], HEADS, width).transpose(1, 0, 2)


def from_heads(stacked):
    return stacked.transpose(1, 0, 2).reshape(stacked.shape[1], stacked.shape[0] * stacked.shape[2])


def reference(query_nope, query_rope, latent, key_rope, key_up, value_up, latent_out, out_grad, logsum, block_order):
    factor = float(NOPE_DIM + ROPE_DIM) ** -0.5
    positions = stored_positions(block_order)
    visible = positions[None, :] <= positions[:, None]

    def one_head(carried, inputs):
        nope_part, rope_part, saved, upstream, key_map, value_map, row_total = inputs
        query_latent = jnp.dot(nope_part, key_map.T, preferred_element_type=jnp.float32).astype(jnp.bfloat16)
        grad_latent = jnp.dot(upstream, value_map.T, preferred_element_type=jnp.float32).astype(jnp.bfloat16)
        scores = (jnp.dot(query_latent, latent.T, preferred_element_type=jnp.float32)
                  + jnp.dot(rope_part, key_rope.T, preferred_element_type=jnp.float32)) * factor
        probs = jnp.where(visible, jnp.exp(jnp.where(visible, scores - row_total, 0.0)), 0.0)
        dprobs = jnp.dot(grad_latent, latent.T, preferred_element_type=jnp.float32)
        row_delta = jnp.sum(grad_latent.astype(jnp.float32) * saved.astype(jnp.float32), axis=1, keepdims=True)
        dscore = (probs * (dprobs - row_delta) * factor).astype(jnp.bfloat16)
        probs_low = probs.astype(jnp.bfloat16)
        grad_query = jnp.dot(dscore, latent, preferred_element_type=jnp.float32).astype(jnp.bfloat16)
        grad_rope = jnp.dot(dscore, key_rope, preferred_element_type=jnp.float32).astype(jnp.bfloat16)
        grad_nope = jnp.dot(grad_query, key_map, preferred_element_type=jnp.float32).astype(jnp.bfloat16)
        latent_sum = (carried[0] + jnp.dot(dscore.T, query_latent, preferred_element_type=jnp.float32)
                      + jnp.dot(probs_low.T, grad_latent, preferred_element_type=jnp.float32))
        rope_sum = carried[1] + jnp.dot(dscore.T, rope_part, preferred_element_type=jnp.float32)
        key_grad = jnp.dot(grad_query.T, nope_part, preferred_element_type=jnp.float32)
        value_grad = jnp.dot(saved.T, upstream, preferred_element_type=jnp.float32)
        return (latent_sum, rope_sum), (grad_nope, grad_rope, key_grad, value_grad)

    start = (jnp.zeros((SEQUENCE, LATENT), jnp.float32), jnp.zeros((SEQUENCE, ROPE_DIM), jnp.float32))
    inputs = (by_head(query_nope, NOPE_DIM), by_head(query_rope, ROPE_DIM), by_head(latent_out, LATENT),
              by_head(out_grad, VALUE_DIM), by_head(key_up, NOPE_DIM), by_head(value_up, VALUE_DIM),
              by_head(logsum, 1))
    sums, stacked = lax.scan(one_head, start, inputs)
    return (from_heads(stacked[0]), from_heads(stacked[1]), sums[0].astype(jnp.bfloat16),
            sums[1].astype(jnp.bfloat16), from_heads(stacked[2]), from_heads(stacked[3]))
```

```python
import jax
import jax.numpy as jnp
from jax import lax
from jax.experimental import pallas as pl
from jax.experimental.pallas import tpu as pltpu
from jax.sharding import Mesh, PartitionSpec as P

LATENT = 512
ROPE_DIM = 64
NOPE_DIM = 128
VALUE_DIM = 128
WIDE = 640
BLOCK = 64
HEADS_HERE = 8
FLAT = BLOCK * HEADS_HERE
TILE = 256
PER_TILE = TILE // BLOCK
FACTOR = float(NOPE_DIM + ROPE_DIM) ** -0.5

f32 = jnp.float32
bf16 = jnp.bfloat16


def dot_nt(a, b):
    return lax.dot_general(a, b, (((1,), (1,)), ((), ())), preferred_element_type=f32)


def dot_nn(a, b):
    return lax.dot_general(a, b, (((1,), (0,)), ((), ())), preferred_element_type=f32)


def dot_tn(a, b):
    return lax.dot_general(a, b, (((0,), (0,)), ((), ())), preferred_element_type=f32)


def split_parity(rows, count, core):
    pieces = rows.reshape(count, 2, rows.shape[0] // (2 * count), rows.shape[1])
    even = pieces[:, 0]
    odd = pieces[:, 1]
    return jnp.where(core == 0, even, odd), jnp.where(core == 0, odd, even)


def prepare_kernel(
    ids, nope, rope, key_up, value_up, saved, upstream, q_out, g_out, delta_out, keep, give
):
    core = ids[1]
    zeros = jnp.zeros((2 * BLOCK, WIDE - LATENT - ROPE_DIM), bf16)
    for h in range(HEADS_HERE):
        cols = slice(h * NOPE_DIM, (h + 1) * NOPE_DIM)
        wide = slice(h * LATENT, (h + 1) * LATENT)
        query = dot_nt(nope[:, cols], key_up[:, cols]).astype(bf16)
        grad = dot_nt(upstream[:, cols], value_up[:, cols]).astype(bf16)
        kept = saved[:, wide]
        delta_out[:, h : h + 1] = jnp.sum(
            grad.astype(f32) * kept.astype(f32), axis=1, keepdims=True
        )
        mine, other = split_parity(dot_tn(kept, upstream[:, cols]), keep.shape[0], core)
        keep[:, :, cols] = mine
        give[:, :, cols] = other.astype(bf16)
        tail = jnp.concatenate([rope[:, h * ROPE_DIM : (h + 1) * ROPE_DIM], zeros], axis=1)
        for j in range(2):
            rows = slice(j * BLOCK, (j + 1) * BLOCK)
            spot = slice(h * BLOCK, (h + 1) * BLOCK)
            q_out[j, spot, :LATENT] = query[rows]
            q_out[j, spot, LATENT:] = tail[rows]
            g_out[j, spot, :] = grad[rows]


def attend_kernel(
    order, ids, keys, q0, g0, v0, q1, g1, v1,
    dk_out, dq_own, dq_peer, where_at, place, seqs, dk_acc, acc_peer,
):
    core = ids[1]
    blocks = order.shape[0]
    chunk = dk_out.shape[1] * 2 * BLOCK // keys.shape[0]
    per_block = BLOCK // chunk

    def note(i, carry):
        where_at[order[i]] = i
        return carry

    lax.fori_loop(0, blocks, note, 0)
    shard = ids[0] * 2
    seq_of = [order[2 * (shard + side) + j] for side in (core, 1 - core) for j in range(2)]

    def pick(s, carry):
        at = where_at[s]
        here = ((at // 2) % 2 == core).astype(jnp.int32)
        place[carry[0]] = (at // 4) * 2 + at % 2
        seqs[carry[0]] = s
        counts = [n + here * (s <= own).astype(jnp.int32) for n, own in zip(carry[1:], seq_of)]
        return (carry[0] + here, *counts)

    counts = lax.fori_loop(0, blocks, pick, (jnp.int32(0),) * 5)[1:]
    dq_own[...] = jnp.zeros(dq_own.shape, f32)
    acc_peer[...] = jnp.zeros(acc_peer.shape, f32)
    key_at = lax.broadcasted_iota(jnp.int32, (BLOCK, FLAT), 0)
    query_at = lax.broadcasted_iota(jnp.int32, (TILE, FLAT), 1) % BLOCK

    def unit(tile, key_pos, qj, gj, vj, acc, j, own):
        scores = dot_nt(tile, qj[j]) * FACTOR
        dprobs = dot_nt(tile[:, :LATENT], gj[j])
        visible = key_pos <= query_at + own * BLOCK
        probs = jnp.exp(jnp.where(visible, scores - vj[j, 0:1, :], -1e30))
        dscore = (probs * (dprobs - vj[j, 1:2, :]) * FACTOR).astype(bf16)
        low_probs = probs.astype(bf16)
        acc[j] += dot_tn(dscore, tile)
        grad = dot_nn(dscore, qj[j])
        dk_acc[:, :LATENT] += grad[:, :LATENT] + dot_nn(low_probs, gj[j])
        dk_acc[:, LATENT:] += grad[:, LATENT:]

    def visit(t, carry):
        spots = [place[t * PER_TILE + i] for i in range(PER_TILE)]
        tile = jnp.concatenate([keys[pl.ds(k * BLOCK, BLOCK), :] for k in spots], axis=0)
        key_pos = jnp.concatenate(
            [key_at + seqs[t * PER_TILE + i] * BLOCK for i in range(PER_TILE)], axis=0
        )
        dk_acc[...] = jnp.zeros(dk_acc.shape, f32)
        sides = ((q0, g0, v0, dq_own), (q1, g1, v1, acc_peer))
        for n in range(4):
            @pl.when(t * PER_TILE < counts[n])
            def _():
                qj, gj, vj, acc = sides[n // 2]
                unit(tile, key_pos, qj, gj, vj, acc, n % 2, seq_of[n])
        for i, k in enumerate(spots):
            for piece in range(per_block):
                at = i * BLOCK + piece * chunk
                dk_out[(k % 2) * per_block + piece, pl.ds((k // 2) * chunk, chunk), :] = dk_acc[
                    at : at + chunk
                ].astype(bf16)
        return carry

    lax.fori_loop(0, keys.shape[0] // TILE, visit, 0)
    dq_peer[...] = acc_peer[...].astype(bf16)


def finish_kernel(ids, dq, dq_add, nope, key_up, dn_out, dr_out, keep, give):
    core = ids[1]
    for h in range(HEADS_HERE):
        cols = slice(h * NOPE_DIM, (h + 1) * NOPE_DIM)
        spot = slice(h * BLOCK, (h + 1) * BLOCK)
        both = [(dq[j, spot] + dq_add[j, spot].astype(f32)).astype(bf16) for j in range(2)]
        whole = jnp.concatenate(both, axis=0)
        grad = whole[:, :LATENT]
        dn_out[:, cols] = dot_nn(grad, key_up[:, cols]).astype(bf16)
        dr_out[:, h * ROPE_DIM : (h + 1) * ROPE_DIM] = whole[:, LATENT : LATENT + ROPE_DIM]
        mine, other = split_parity(dot_tn(grad, nope[:, cols]), keep.shape[0], core)
        keep[:, :, cols] = mine
        give[:, :, cols] = other.astype(bf16)


def in_vmem(count):
    return [pl.BlockSpec(memory_space=pltpu.VMEM)] * count


def in_smem(count):
    return [pl.BlockSpec(memory_space=pltpu.SMEM)] * count


def shape(dims, dtype):
    return jax.ShapeDtypeStruct(dims, dtype)


IZ = ("inner", "z")
GRP = ("inner", "z", "core")


def to_partner(x):
    return lax.ppermute(x, "core", [(0, 1), (1, 0)])


def exchange(x, axis):
    return lax.all_to_all(x, axis, split_axis=0, concat_axis=0, tiled=True)


def local(
    query_nope,
    query_rope,
    latent,
    key_rope,
    key_up,
    value_up,
    latent_out,
    out_grad,
    logsum,
    block_order,
):
    tokens = query_nope.shape[0]
    sets = lax.axis_size(IZ)
    heads = lax.axis_size("head")
    weight_rows = LATENT // (2 * sets)
    half = (sets, weight_rows, HEADS_HERE * NOPE_DIM)
    params = pltpu.CompilerParams(vmem_limit_bytes=58 * 1024 * 1024)
    ids = jnp.stack([lax.axis_index(IZ), lax.axis_index("core")]).astype(jnp.int32)
    mine = jnp.concatenate(
        [latent, key_rope, jnp.zeros((tokens, WIDE - LATENT - ROPE_DIM), bf16)], axis=1
    )
    keys = lax.all_gather(mine, IZ, axis=0, tiled=True)
    q, g, delta, value_keep, value_give = pl.pallas_call(
        prepare_kernel,
        in_specs=in_smem(1) + in_vmem(6),
        out_specs=in_vmem(5),
        out_shape=[
            shape((2, FLAT, WIDE), bf16),
            shape((2, FLAT, LATENT), bf16),
            shape((tokens, HEADS_HERE), f32),
            shape(half, f32),
            shape(half, bf16),
        ],
        compiler_params=params,
        name="prepare",
    )(ids, query_nope, query_rope, key_up, value_up, latent_out, out_grad)
    row_vals = jnp.stack([logsum, delta]).reshape(2, 2, BLOCK, HEADS_HERE)
    row_vals = row_vals.transpose(1, 0, 3, 2).reshape(2, 2, FLAT)
    q_peer, g_peer, vals_peer = to_partner(q), to_partner(g), to_partner(row_vals)
    value_part = (value_keep + to_partner(value_give).astype(f32)).astype(bf16)
    value_parts = exchange(value_part, IZ)
    value_parts, row_vals = lax.optimization_barrier((value_parts, row_vals))
    dk, dq, dq_give = pl.pallas_call(
        attend_kernel,
        in_specs=in_smem(2) + in_vmem(7),
        out_specs=in_vmem(3),
        out_shape=[
            shape((heads, sets * tokens // heads, WIDE), bf16),
            shape((2, FLAT, WIDE), f32),
            shape((2, FLAT, WIDE), bf16),
        ],
        scratch_shapes=[
            pltpu.SMEM((block_order.shape[0],), jnp.int32),
            pltpu.SMEM((block_order.shape[0],), jnp.int32),
            pltpu.SMEM((block_order.shape[0],), jnp.int32),
            pltpu.VMEM((TILE, WIDE), f32),
            pltpu.VMEM((2, FLAT, WIDE), f32),
        ],
        compiler_params=params,
        name="attend",
    )(block_order, ids, keys, q, g, row_vals, q_peer, g_peer, vals_peer)
    by_head = jnp.sum(exchange(dk, "head").astype(f32), axis=0).astype(bf16)
    dq_add = to_partner(dq_give)
    d_nope, d_rope, key_keep, key_give = pl.pallas_call(
        finish_kernel,
        in_specs=in_smem(1) + in_vmem(4),
        out_specs=in_vmem(4),
        out_shape=[
            shape(query_nope.shape, bf16),
            shape(query_rope.shape, bf16),
            shape(half, f32),
            shape(half, bf16),
        ],
        compiler_params=params,
        name="finish",
    )(ids, dq, dq_add, query_nope, key_up)
    by_set = exchange(by_head.reshape(sets, tokens // heads, WIDE), IZ)
    owned = jnp.sum(by_set.astype(f32), axis=0).astype(bf16)
    total = exchange(jnp.broadcast_to(owned, (heads, *owned.shape)), "head").reshape(tokens, WIDE)
    key_part = (key_keep + to_partner(key_give).astype(f32)).astype(bf16)
    key_grad = jnp.sum(exchange(key_part, IZ).astype(f32), axis=0)
    value_grad = jnp.sum(value_parts.astype(f32), axis=0)
    return (
        d_nope,
        d_rope,
        total[:, :LATENT],
        total[:, LATENT : LATENT + ROPE_DIM],
        key_grad,
        value_grad,
    )


def solution(mesh):
    heads, inner, outer = mesh.devices.shape
    fine = Mesh(
        mesh.devices.reshape(heads, inner, outer // 2, 2), ("head", "inner", "z", "core")
    )
    rows = P(GRP, "head")
    return jax.shard_map(
        local,
        mesh=fine,
        in_specs=(rows, rows, P(GRP, None), P(GRP, None), P(None, "head"), P(None, "head"),
                  rows, rows, rows, P()),
        out_specs=(rows, rows, P(GRP, None), P(GRP, None), rows, rows),
        check_vma=False,
    )
```

```python
import jax
import jax.numpy as jnp
from jax import lax
from jax.experimental import pallas as pl
from jax.experimental.pallas import tpu as pltpu
from jax.sharding import Mesh, PartitionSpec as P

LATENT = 512
ROPE_DIM = 64
NOPE_DIM = 128
VALUE_DIM = 128
WIDE = 640
BLOCK = 64
HEADS_HERE = 8
FLAT = BLOCK * HEADS_HERE
TILE = 256
PER_TILE = TILE // BLOCK
FACTOR = float(NOPE_DIM + ROPE_DIM) ** -0.5

f32 = jnp.float32
bf16 = jnp.bfloat16


def dot_nt(a, b):
    return lax.dot_general(a, b, (((1,), (1,)), ((), ())), preferred_element_type=f32)


def dot_nn(a, b):
    return lax.dot_general(a, b, (((1,), (0,)), ((), ())), preferred_element_type=f32)


def dot_tn(a, b):
    return lax.dot_general(a, b, (((0,), (0,)), ((), ())), preferred_element_type=f32)


def split_parity(rows, count, core):
    pieces = rows.reshape(count, 2, rows.shape[0] // (2 * count), rows.shape[1])
    even = pieces[:, 0]
    odd = pieces[:, 1]
    return jnp.where(core == 0, even, odd), jnp.where(core == 0, odd, even)


def prepare_kernel(
    ids, nope, rope, key_up, value_up, saved, upstream, q_out, g_out, delta_out, keep, give
):
    core = ids[1]
    zeros = jnp.zeros((2 * BLOCK, WIDE - LATENT - ROPE_DIM), bf16)
    for h in range(HEADS_HERE):
        cols = slice(h * NOPE_DIM, (h + 1) * NOPE_DIM)
        wide = slice(h * LATENT, (h + 1) * LATENT)
        query = dot_nt(nope[:, cols], key_up[:, cols]).astype(bf16)
        grad = dot_nt(upstream[:, cols], value_up[:, cols]).astype(bf16)
        kept = saved[:, wide]
        delta_out[:, h : h + 1] = jnp.sum(
            grad.astype(f32) * kept.astype(f32), axis=1, keepdims=True
        )
        mine, other = split_parity(dot_tn(kept, upstream[:, cols]), keep.shape[0], core)
        keep[:, :, cols] = mine
        give[:, :, cols] = other.astype(bf16)
        tail = jnp.concatenate([rope[:, h * ROPE_DIM : (h + 1) * ROPE_DIM], zeros], axis=1)
        for j in range(2):
            rows = slice(j * BLOCK, (j + 1) * BLOCK)
            spot = slice(h * BLOCK, (h + 1) * BLOCK)
            q_out[j, spot, :LATENT] = query[rows]
            q_out[j, spot, LATENT:] = tail[rows]
            g_out[j, spot, :] = grad[rows]


def attend_kernel(
    order, ids, keys, q0, g0, v0, q1, g1, v1,
    dk_out, dq_own, dq_peer, where_at, place, seqs, dk_acc, acc_peer,
):
    core = ids[1]
    blocks = order.shape[0]
    per_block = keys.shape[0] // 2
    chunk = BLOCK // per_block

    def note(i, carry):
        where_at[order[i]] = i
        return carry

    lax.fori_loop(0, blocks, note, 0)
    shard = ids[0] * 2
    seq_of = [order[2 * (shard + side) + j] for side in (core, 1 - core) for j in range(2)]

    def pick(s, carry):
        at = where_at[s]
        here = ((at // 2) % 2 == core).astype(jnp.int32)
        place[carry[0]] = (at // 4) * 2 + at % 2
        seqs[carry[0]] = s
        counts = [n + here * (s <= own).astype(jnp.int32) for n, own in zip(carry[1:], seq_of)]
        return (carry[0] + here, *counts)

    counts = lax.fori_loop(0, blocks, pick, (jnp.int32(0),) * 5)[1:]
    dq_own[...] = jnp.zeros(dq_own.shape, f32)
    acc_peer[...] = jnp.zeros(acc_peer.shape, f32)
    key_at = lax.broadcasted_iota(jnp.int32, (BLOCK, FLAT), 0)
    query_at = lax.broadcasted_iota(jnp.int32, (TILE, FLAT), 1) % BLOCK

    def unit(tile, key_pos, qj, gj, vj, acc, j, own):
        scores = dot_nt(tile, qj[j]) * FACTOR
        dprobs = dot_nt(tile[:, :LATENT], gj[j])
        visible = key_pos <= query_at + own * BLOCK
        probs = jnp.exp(jnp.where(visible, scores - vj[j, 0:1, :], -1e30))
        dscore = (probs * (dprobs - vj[j, 1:2, :]) * FACTOR).astype(bf16)
        low_probs = probs.astype(bf16)
        acc[j] += dot_tn(dscore, tile)
        grad = dot_nn(dscore, qj[j])
        dk_acc[:, :LATENT] += grad[:, :LATENT] + dot_nn(low_probs, gj[j])
        dk_acc[:, LATENT:] += grad[:, LATENT:]

    def visit(t, carry):
        spots = [place[t * PER_TILE + i] for i in range(PER_TILE)]
        pieces = [
            ((k % 2) * per_block + piece, pl.ds((k // 2) * chunk, chunk))
            for k in spots
            for piece in range(per_block)
        ]
        tile = jnp.concatenate([keys[h, rows, :] for h, rows in pieces], axis=0)
        key_pos = jnp.concatenate(
            [key_at + seqs[t * PER_TILE + i] * BLOCK for i in range(PER_TILE)], axis=0
        )
        dk_acc[...] = jnp.zeros(dk_acc.shape, f32)
        sides = ((q0, g0, v0, dq_own), (q1, g1, v1, acc_peer))
        for n in range(4):
            @pl.when(t * PER_TILE < counts[n])
            def _():
                qj, gj, vj, acc = sides[n // 2]
                unit(tile, key_pos, qj, gj, vj, acc, n % 2, seq_of[n])
        for n, (h, rows) in enumerate(pieces):
            dk_out[h, rows, :] = dk_acc[n * chunk : (n + 1) * chunk].astype(bf16)
        return carry

    lax.fori_loop(0, keys.shape[0] * keys.shape[1] // TILE, visit, 0)
    dq_peer[...] = acc_peer[...].astype(bf16)


def finish_kernel(ids, dq, dq_add, nope, key_up, dn_out, dr_out, keep, give):
    core = ids[1]
    for h in range(HEADS_HERE):
        cols = slice(h * NOPE_DIM, (h + 1) * NOPE_DIM)
        spot = slice(h * BLOCK, (h + 1) * BLOCK)
        both = [(dq[j, spot] + dq_add[j, spot].astype(f32)).astype(bf16) for j in range(2)]
        whole = jnp.concatenate(both, axis=0)
        grad = whole[:, :LATENT]
        dn_out[:, cols] = dot_nn(grad, key_up[:, cols]).astype(bf16)
        dr_out[:, h * ROPE_DIM : (h + 1) * ROPE_DIM] = whole[:, LATENT : LATENT + ROPE_DIM]
        mine, other = split_parity(dot_tn(grad, nope[:, cols]), keep.shape[0], core)
        keep[:, :, cols] = mine
        give[:, :, cols] = other.astype(bf16)


def in_vmem(count):
    return [pl.BlockSpec(memory_space=pltpu.VMEM)] * count


def in_smem(count):
    return [pl.BlockSpec(memory_space=pltpu.SMEM)] * count


def shape(dims, dtype):
    return jax.ShapeDtypeStruct(dims, dtype)


IZ = ("inner", "z")
GRP = ("inner", "z", "core")


def to_partner(x):
    return lax.ppermute(x, "core", [(0, 1), (1, 0)])


def exchange(x, axis):
    return lax.all_to_all(x, axis, split_axis=0, concat_axis=0, tiled=True)


def to_all(x, axis):
    return exchange(jnp.broadcast_to(x, (lax.axis_size(axis), *x.shape)), axis)


def local(
    query_nope,
    query_rope,
    latent,
    key_rope,
    key_up,
    value_up,
    latent_out,
    out_grad,
    logsum,
    block_order,
):
    tokens = query_nope.shape[0]
    sets = lax.axis_size(IZ)
    heads = lax.axis_size("head")
    weight_rows = LATENT // (2 * sets)
    half = (sets, weight_rows, HEADS_HERE * NOPE_DIM)
    params = pltpu.CompilerParams(vmem_limit_bytes=58 * 1024 * 1024)
    ids = jnp.stack([lax.axis_index(IZ), lax.axis_index("core")]).astype(jnp.int32)
    chunk = tokens // heads
    first = lax.axis_index("head") * chunk
    mine = jnp.concatenate(
        [
            lax.dynamic_slice_in_dim(latent, first, chunk, 0),
            lax.dynamic_slice_in_dim(key_rope, first, chunk, 0),
            jnp.zeros((chunk, WIDE - LATENT - ROPE_DIM), bf16),
        ],
        axis=1,
    )
    slices = to_all(mine, IZ).reshape(sets * chunk, WIDE)
    keys = to_all(slices, "head")
    q, g, delta, value_keep, value_give = pl.pallas_call(
        prepare_kernel,
        in_specs=in_smem(1) + in_vmem(6),
        out_specs=in_vmem(5),
        out_shape=[
            shape((2, FLAT, WIDE), bf16),
            shape((2, FLAT, LATENT), bf16),
            shape((tokens, HEADS_HERE), f32),
            shape(half, f32),
            shape(half, bf16),
        ],
        compiler_params=params,
        name="prepare",
    )(ids, query_nope, query_rope, key_up, value_up, latent_out, out_grad)
    row_vals = jnp.stack([logsum, delta]).reshape(2, 2, BLOCK, HEADS_HERE)
    row_vals = row_vals.transpose(1, 0, 3, 2).reshape(2, 2, FLAT)
    q_peer, g_peer, vals_peer = to_partner(q), to_partner(g), to_partner(row_vals)
    value_part = (value_keep + to_partner(value_give).astype(f32)).astype(bf16)
    value_part, *_ = lax.optimization_barrier((value_part, keys, q_peer, g_peer, vals_peer))
    value_parts = exchange(value_part, IZ)
    attend = pl.pallas_call(
        attend_kernel,
        in_specs=in_smem(2) + in_vmem(7),
        out_specs=in_vmem(3),
        out_shape=[
            shape((heads, sets * chunk, WIDE), bf16),
            shape((2, FLAT, WIDE), f32),
            shape((2, FLAT, WIDE), bf16),
        ],
        scratch_shapes=[
            pltpu.SMEM((block_order.shape[0],), jnp.int32),
            pltpu.SMEM((block_order.shape[0],), jnp.int32),
            pltpu.SMEM((block_order.shape[0],), jnp.int32),
            pltpu.VMEM((TILE, WIDE), f32),
            pltpu.VMEM((2, FLAT, WIDE), f32),
        ],
        compiler_params=params,
        name="attend",
    )
    dk, dq, dq_give = attend(block_order, ids, keys, q, g, row_vals, q_peer, g_peer, vals_peer)
    dk, value_parts = lax.optimization_barrier((dk, value_parts))
    by_head = jnp.sum(exchange(dk, "head").astype(f32), axis=0).astype(bf16)
    dq_add = to_partner(dq_give)
    d_nope, d_rope, key_keep, key_give = pl.pallas_call(
        finish_kernel,
        in_specs=in_smem(1) + in_vmem(4),
        out_specs=in_vmem(4),
        out_shape=[
            shape(query_nope.shape, bf16),
            shape(query_rope.shape, bf16),
            shape(half, f32),
            shape(half, bf16),
        ],
        compiler_params=params,
        name="finish",
    )(ids, dq, dq_add, query_nope, key_up)
    key_part = (key_keep + to_partner(key_give).astype(f32)).astype(bf16)
    joined = jnp.concatenate([by_head.reshape(sets, chunk, WIDE), key_part], axis=2)
    by_set = exchange(joined, IZ)
    owned = jnp.sum(by_set[:, :, :WIDE].astype(f32), axis=0).astype(bf16)
    key_grad = jnp.sum(by_set[:, :, WIDE:].astype(f32), axis=0)
    total = to_all(owned, "head").reshape(tokens, WIDE)
    value_grad = jnp.sum(value_parts.astype(f32), axis=0)
    return (
        d_nope,
        d_rope,
        total[:, :LATENT],
        total[:, LATENT : LATENT + ROPE_DIM],
        key_grad,
        value_grad,
    )


def solution(mesh):
    heads, inner, outer = mesh.devices.shape
    fine = Mesh(
        mesh.devices.reshape(heads, inner, outer // 2, 2), ("head", "inner", "z", "core")
    )
    rows = P(GRP, "head")
    return jax.shard_map(
        local,
        mesh=fine,
        in_specs=(rows, rows, P(GRP, None), P(GRP, None), P(None, "head"), P(None, "head"),
                  rows, rows, rows, P()),
        out_specs=(rows, rows, P(GRP, None), P(GRP, None), rows, rows),
        check_vma=False,
    )
```

```python
import jax
import jax.numpy as jnp
from jax import lax
from jax.experimental import pallas as pl
from jax.experimental.pallas import tpu as pltpu
from jax.sharding import Mesh, PartitionSpec as P

LATENT = 512
ROPE_DIM = 64
NOPE_DIM = 128
WIDE = 640
BLOCK = 64
HEADS_HERE = 8
FLAT = BLOCK * HEADS_HERE
TILE = 256
PER_TILE = TILE // BLOCK
FACTOR = float(NOPE_DIM + ROPE_DIM) ** -0.5

f32 = jnp.float32
bf16 = jnp.bfloat16


def dot_nt(a, b):
    return lax.dot_general(a, b, (((1,), (1,)), ((), ())), preferred_element_type=f32)


def dot_nn(a, b):
    return lax.dot_general(a, b, (((1,), (0,)), ((), ())), preferred_element_type=f32)


def dot_tn(a, b):
    return lax.dot_general(a, b, (((0,), (0,)), ((), ())), preferred_element_type=f32)


def split_parity(rows, count, core):
    pieces = rows.reshape(count, 2, rows.shape[0] // (2 * count), rows.shape[1])
    even = pieces[:, 0]
    odd = pieces[:, 1]
    return jnp.where(core == 0, even, odd), jnp.where(core == 0, odd, even)


def prepare_kernel(
    ids, nope, rope, key_up, value_up, saved, upstream, q_out, g_out, delta_out, keep, give
):
    core = ids[1]
    zeros = jnp.zeros((2 * BLOCK, WIDE - LATENT - ROPE_DIM), bf16)
    for h in range(HEADS_HERE):
        cols = slice(h * NOPE_DIM, (h + 1) * NOPE_DIM)
        wide = slice(h * LATENT, (h + 1) * LATENT)
        query = dot_nt(nope[:, cols], key_up[:, cols]).astype(bf16)
        grad = dot_nt(upstream[:, cols], value_up[:, cols]).astype(bf16)
        kept = saved[:, wide]
        delta_out[:, h : h + 1] = jnp.sum(
            grad.astype(f32) * kept.astype(f32), axis=1, keepdims=True
        )
        mine, other = split_parity(dot_tn(kept, upstream[:, cols]), keep.shape[0], core)
        keep[:, :, cols] = mine
        give[:, :, cols] = other.astype(bf16)
        tail = jnp.concatenate([rope[:, h * ROPE_DIM : (h + 1) * ROPE_DIM], zeros], axis=1)
        for j in range(2):
            rows = slice(j * BLOCK, (j + 1) * BLOCK)
            spot = slice(h * BLOCK, (h + 1) * BLOCK)
            q_out[j, spot, :LATENT] = query[rows]
            q_out[j, spot, LATENT:] = tail[rows]
            g_out[j, spot, :] = grad[rows]


def attend_kernel(
    order, ids, keys, q0, g0, v0, q1, g1, v1,
    dk_out, dq_own, dq_peer, where_at, place, seqs, dk_acc, acc_own, acc_peer,
):
    core = ids[1]
    blocks = order.shape[0]
    per_block = keys.shape[0] // 2
    chunk = BLOCK // per_block

    def note(i, carry):
        where_at[order[i]] = i
        return carry

    lax.fori_loop(0, blocks, note, 0)
    shard = ids[0] * 2
    seq_of = [order[2 * (shard + side) + j] for side in (core, 1 - core) for j in range(2)]

    def pick(s, carry):
        at = where_at[s]
        here = ((at // 2) % 2 == core).astype(jnp.int32)
        place[carry[0]] = (at // 4) * 2 + at % 2
        seqs[carry[0]] = s
        counts = [n + here * (s <= own).astype(jnp.int32) for n, own in zip(carry[1:], seq_of)]
        return (carry[0] + here, *counts)

    counts = lax.fori_loop(0, blocks, pick, (jnp.int32(0),) * 5)[1:]
    acc_own[...] = jnp.zeros(acc_own.shape, f32)
    acc_peer[...] = jnp.zeros(acc_peer.shape, f32)
    key_at = lax.broadcasted_iota(jnp.int32, (BLOCK, FLAT), 0)
    query_at = lax.broadcasted_iota(jnp.int32, (TILE, FLAT), 1) % BLOCK

    def unit(tile, key_pos, qj, gj, vj, acc, j, own):
        scores = dot_nt(tile, qj[j]) * FACTOR
        dprobs = dot_nt(tile[:, :LATENT], gj[j])
        visible = key_pos <= query_at + own * BLOCK
        probs = jnp.exp(jnp.where(visible, scores - vj[j, 0:1, :], -1e30))
        dscore = (probs * (dprobs - vj[j, 1:2, :]) * FACTOR).astype(bf16)
        low_probs = probs.astype(bf16)
        acc[j] += dot_tn(dscore, tile)
        grad = dot_nn(dscore, qj[j])
        dk_acc[:, :LATENT] += grad[:, :LATENT] + dot_nn(low_probs, gj[j])
        dk_acc[:, LATENT:] += grad[:, LATENT:]

    def visit(t, carry):
        spots = [place[t * PER_TILE + i] for i in range(PER_TILE)]
        pieces = [
            ((k % 2) * per_block + piece, pl.ds((k // 2) * chunk, chunk))
            for k in spots
            for piece in range(per_block)
        ]
        tile = jnp.concatenate([keys[h, rows, :] for h, rows in pieces], axis=0)
        key_pos = jnp.concatenate(
            [key_at + seqs[t * PER_TILE + i] * BLOCK for i in range(PER_TILE)], axis=0
        )
        dk_acc[...] = jnp.zeros(dk_acc.shape, f32)
        sides = ((q0, g0, v0, acc_own), (q1, g1, v1, acc_peer))
        for n in range(4):
            @pl.when(t * PER_TILE < counts[n])
            def _():
                qj, gj, vj, acc = sides[n // 2]
                unit(tile, key_pos, qj, gj, vj, acc, n % 2, seq_of[n])
        for n, (h, rows) in enumerate(pieces):
            dk_out[h, rows, :] = dk_acc[n * chunk : (n + 1) * chunk].astype(bf16)
        return carry

    lax.fori_loop(0, keys.shape[0] * keys.shape[1] // TILE, visit, 0)
    dq_own[...] = acc_own[...].astype(bf16)
    dq_peer[...] = acc_peer[...].astype(bf16)


def finish_kernel(ids, dq, dq_add, nope, key_up, dn_out, dr_out, keep, give):
    core = ids[1]
    for h in range(HEADS_HERE):
        cols = slice(h * NOPE_DIM, (h + 1) * NOPE_DIM)
        spot = slice(h * BLOCK, (h + 1) * BLOCK)
        both = [(dq[j, spot].astype(f32) + dq_add[j, spot].astype(f32)).astype(bf16) for j in range(2)]
        whole = jnp.concatenate(both, axis=0)
        grad = whole[:, :LATENT]
        dn_out[:, cols] = dot_nn(grad, key_up[:, cols]).astype(bf16)
        dr_out[:, h * ROPE_DIM : (h + 1) * ROPE_DIM] = whole[:, LATENT : LATENT + ROPE_DIM]
        mine, other = split_parity(dot_tn(grad, nope[:, cols]), keep.shape[0], core)
        keep[:, :, cols] = mine
        give[:, :, cols] = other.astype(bf16)


def in_vmem(count):
    return [pl.BlockSpec(memory_space=pltpu.VMEM)] * count


def in_smem(count):
    return [pl.BlockSpec(memory_space=pltpu.SMEM)] * count


def shape(dims, dtype):
    return jax.ShapeDtypeStruct(dims, dtype)


IZ = ("inner", "z")
GRP = ("inner", "z", "core")


def to_partner(x):
    return lax.ppermute(x, "core", [(0, 1), (1, 0)])


def exchange(x, axis):
    return lax.all_to_all(x, axis, split_axis=0, concat_axis=0, tiled=True)


def to_all(x, axis):
    return exchange(jnp.broadcast_to(x, (lax.axis_size(axis), *x.shape)), axis)


def whole(
    query_nope,
    query_rope,
    latent,
    key_rope,
    key_up,
    value_up,
    latent_out,
    out_grad,
    logsum,
    block_order,
):
    tokens = query_nope.shape[0]
    sets = lax.axis_size(IZ)
    heads = lax.axis_size("head")
    weight_rows = LATENT // (2 * sets)
    half = (sets, weight_rows, HEADS_HERE * NOPE_DIM)
    params = pltpu.CompilerParams(vmem_limit_bytes=58 * 1024 * 1024)
    ids = jnp.stack([lax.axis_index(IZ), lax.axis_index("core")]).astype(jnp.int32)
    chunk = tokens // heads
    first = lax.axis_index("head") * chunk
    mine = jnp.concatenate(
        [
            lax.dynamic_slice_in_dim(latent, first, chunk, 0),
            lax.dynamic_slice_in_dim(key_rope, first, chunk, 0),
            jnp.zeros((chunk, WIDE - LATENT - ROPE_DIM), bf16),
        ],
        axis=1,
    )
    slices = to_all(mine, IZ).reshape(sets * chunk, WIDE)
    prepare = pl.pallas_call(
        prepare_kernel,
        in_specs=in_smem(1) + in_vmem(6),
        out_specs=in_vmem(5),
        out_shape=[
            shape((2, FLAT, WIDE), bf16),
            shape((2, FLAT, LATENT), bf16),
            shape((tokens, HEADS_HERE), f32),
            shape(half, f32),
            shape(half, bf16),
        ],
        compiler_params=params,
        name="prepare",
    )
    q, g, delta, value_keep, value_give = prepare(
        ids, query_nope, query_rope, key_up, value_up, latent_out, out_grad
    )
    row_vals = jnp.stack([logsum, delta]).reshape(2, 2, BLOCK, HEADS_HERE)
    row_vals = row_vals.transpose(1, 0, 3, 2).reshape(2, 2, FLAT)
    q_peer, g_peer, vals_peer = to_partner(q), to_partner(g), to_partner(row_vals)
    value_part = (value_keep + to_partner(value_give).astype(f32)).astype(bf16)
    slices, value_part, q_peer, g_peer, vals_peer = lax.optimization_barrier(
        (slices, value_part, q_peer, g_peer, vals_peer)
    )
    keys = to_all(slices, "head")
    value_part, _ = lax.optimization_barrier((value_part, keys))
    value_parts = exchange(value_part, IZ)
    attend = pl.pallas_call(
        attend_kernel,
        in_specs=in_smem(2) + in_vmem(7),
        out_specs=in_vmem(3),
        out_shape=[
            shape((heads, sets * chunk, WIDE), bf16),
            shape((2, FLAT, WIDE), bf16),
            shape((2, FLAT, WIDE), bf16),
        ],
        scratch_shapes=[
            pltpu.SMEM((block_order.shape[0],), jnp.int32),
            pltpu.SMEM((block_order.shape[0],), jnp.int32),
            pltpu.SMEM((block_order.shape[0],), jnp.int32),
            pltpu.VMEM((TILE, WIDE), f32),
            pltpu.VMEM((2, FLAT, WIDE), f32),
            pltpu.VMEM((2, FLAT, WIDE), f32),
        ],
        compiler_params=params,
        name="attend",
    )
    dk, dq, dq_give = attend(block_order, ids, keys, q, g, row_vals, q_peer, g_peer, vals_peer)
    dk, value_parts = lax.optimization_barrier((dk, value_parts))
    by_head = jnp.sum(exchange(dk, "head").astype(f32), axis=0).astype(bf16)
    dq_add = to_partner(dq_give)
    d_nope, d_rope, key_keep, key_give = pl.pallas_call(
        finish_kernel,
        in_specs=in_smem(1) + in_vmem(4),
        out_specs=in_vmem(4),
        out_shape=[
            shape(query_nope.shape, bf16),
            shape(query_rope.shape, bf16),
            shape(half, f32),
            shape(half, bf16),
        ],
        compiler_params=params,
        name="finish",
    )(ids, dq, dq_add, query_nope, key_up)
    key_part = (key_keep + to_partner(key_give).astype(f32)).astype(bf16)
    joined = jnp.concatenate([by_head.reshape(sets, chunk, WIDE), key_part], axis=2)
    by_set = exchange(joined, IZ)
    owned = jnp.sum(by_set[:, :, :WIDE].astype(f32), axis=0).astype(bf16)
    key_grad = jnp.sum(by_set[:, :, WIDE:].astype(f32), axis=0)
    total = to_all(owned, "head").reshape(tokens, WIDE)
    value_grad = jnp.sum(value_parts.astype(f32), axis=0)
    return (
        d_nope,
        d_rope,
        total[:, :LATENT],
        total[:, LATENT : LATENT + ROPE_DIM],
        key_grad,
        value_grad,
    )


def solution(mesh):
    heads, inner, outer = mesh.devices.shape
    fine = Mesh(
        mesh.devices.reshape(heads, inner, outer // 2, 2), ("head", "inner", "z", "core")
    )
    rows = P(GRP, "head")
    return jax.shard_map(
        whole,
        mesh=fine,
        in_specs=(rows, rows, P(GRP, None), P(GRP, None), P(None, "head"), P(None, "head"),
                  rows, rows, rows, P()),
        out_specs=(rows, rows, P(GRP, None), P(GRP, None), rows, rows),
        check_vma=False,
    )
```

```python
import jax
import jax.numpy as jnp
from jax import lax
from jax.experimental import pallas as pl
from jax.experimental.pallas import tpu as pltpu
from jax.sharding import Mesh, PartitionSpec as P

LATENT = 512
ROPE_DIM = 64
NOPE_DIM = 128
VALUE_DIM = 128
WIDE = 640
BLOCK = 64
HEADS_HERE = 8
FLAT = BLOCK * HEADS_HERE
TILE = 512
LANES = 128
SLABS = LATENT // LANES
PER_TILE = TILE // BLOCK
FACTOR = float(NOPE_DIM + ROPE_DIM) ** -0.5

f32 = jnp.float32
bf16 = jnp.bfloat16


def dot_nt(a, b):
    return lax.dot_general(a, b, (((1,), (1,)), ((), ())), preferred_element_type=f32)


def dot_nn(a, b):
    return lax.dot_general(a, b, (((1,), (0,)), ((), ())), preferred_element_type=f32)


def dot_tn(a, b):
    return lax.dot_general(a, b, (((0,), (0,)), ((), ())), preferred_element_type=f32)


def split_parity(rows, count, core):
    pieces = rows.reshape(count, 2, rows.shape[0] // (2 * count), rows.shape[1])
    even = pieces[:, 0]
    odd = pieces[:, 1]
    return jnp.where(core == 0, even, odd), jnp.where(core == 0, odd, even)


def prepare_kernel(
    ids, nope, rope, key_up, value_up, saved, upstream, q_out, g_out, delta_out, keep, give
):
    core = ids[1]
    zeros = jnp.zeros((2 * BLOCK, WIDE - LATENT - ROPE_DIM), bf16)
    for h in range(HEADS_HERE):
        cols = slice(h * NOPE_DIM, (h + 1) * NOPE_DIM)
        wide = slice(h * LATENT, (h + 1) * LATENT)
        query = dot_nt(nope[:, cols], key_up[:, cols]).astype(bf16)
        grad = dot_nt(upstream[:, cols], value_up[:, cols]).astype(bf16)
        kept = saved[:, wide]
        delta_out[:, h : h + 1] = jnp.sum(
            grad.astype(f32) * kept.astype(f32), axis=1, keepdims=True
        )
        mine, other = split_parity(dot_tn(kept, upstream[:, cols]), keep.shape[0], core)
        slab = slice(h * mine.shape[1], (h + 1) * mine.shape[1])
        keep[:, slab, :] = mine
        give[:, slab, :] = other.astype(bf16)
        tail = jnp.concatenate([rope[:, h * ROPE_DIM : (h + 1) * ROPE_DIM], zeros], axis=1)
        for j in range(2):
            rows = slice(j * BLOCK, (j + 1) * BLOCK)
            spot = slice(h * BLOCK, (h + 1) * BLOCK)
            q_out[j, spot, :LATENT] = query[rows]
            q_out[j, spot, LATENT:] = tail[rows]
            g_out[j, spot, :] = grad[rows]


def attend_kernel(
    order, ids, keys, q0, g0, v0, q1, g1, v1,
    dk_out, dq_own, dq_peer, where_at, place, seqs, dk_acc, acc_own, acc_peer,
):
    core = ids[1]
    blocks = order.shape[0]
    per_block = keys.shape[0] // 2
    chunk = BLOCK // per_block

    def note(i, carry):
        where_at[order[i]] = i
        return carry

    lax.fori_loop(0, blocks, note, 0)
    shard = ids[0] * 2
    seq_of = [order[2 * (shard + side) + j] for side in (core, 1 - core) for j in range(2)]

    def pick(s, carry):
        at = where_at[s]
        here = ((at // 2) % 2 == core).astype(jnp.int32)
        place[carry[0]] = (at // 4) * 2 + at % 2
        seqs[carry[0]] = s
        counts = [n + here * (s <= own).astype(jnp.int32) for n, own in zip(carry[1:], seq_of)]
        return (carry[0] + here, *counts)

    counts = lax.fori_loop(0, blocks, pick, (jnp.int32(0),) * 5)[1:]
    acc_own[...] = jnp.zeros(acc_own.shape, f32)
    acc_peer[...] = jnp.zeros(acc_peer.shape, f32)
    key_at = lax.broadcasted_iota(jnp.int32, (BLOCK, FLAT), 0)
    query_at = lax.broadcasted_iota(jnp.int32, (TILE, FLAT), 1) % BLOCK

    def unit(tile, key_pos, qj, gj, vj, acc, j, own):
        scores = dot_nt(tile, qj[j]) * FACTOR
        dprobs = dot_nt(tile[:, :LATENT], gj[j])
        visible = key_pos <= query_at + own * BLOCK
        probs = jnp.exp(jnp.where(visible, scores - vj[j, 0:1, :], -1e30))
        dscore = (probs * (dprobs - vj[j, 1:2, :]) * FACTOR).astype(bf16)
        low_probs = probs.astype(bf16)
        acc[j] += dot_tn(dscore, tile)
        grad = dot_nn(dscore, qj[j])
        dk_acc[:, :LATENT] += grad[:, :LATENT] + dot_nn(low_probs, gj[j])
        dk_acc[:, LATENT:] += grad[:, LATENT:]

    def unpack(h, s):
        slabs = [keys[h, s, i * chunk : (i + 1) * chunk, :] for i in range(SLABS)]
        rot = keys[h, s, SLABS * chunk :, :].astype(f32)
        both = jnp.concatenate([rot, pltpu.roll(rot, ROPE_DIM, 1)], axis=0).astype(bf16)
        return jnp.concatenate([*slabs, both], axis=1)

    def visit(t, carry):
        spots = [place[t * PER_TILE + i] for i in range(PER_TILE)]
        pieces = [
            ((k % 2) * per_block + piece, k // 2) for k in spots for piece in range(per_block)
        ]
        tile = jnp.concatenate([unpack(h, s) for h, s in pieces], axis=0)
        key_pos = jnp.concatenate(
            [key_at + seqs[t * PER_TILE + i] * BLOCK for i in range(PER_TILE)], axis=0
        )
        dk_acc[...] = jnp.zeros(dk_acc.shape, f32)
        sides = ((q0, g0, v0, acc_own), (q1, g1, v1, acc_peer))
        for n in range(4):
            @pl.when(t * PER_TILE < counts[n])
            def _():
                qj, gj, vj, acc = sides[n // 2]
                unit(tile, key_pos, qj, gj, vj, acc, n % 2, seq_of[n])
        for n, (h, s) in enumerate(pieces):
            part = dk_acc[n * chunk : (n + 1) * chunk]
            for i in range(SLABS):
                dk_out[h, s, i * chunk : (i + 1) * chunk, :] = part[
                    :, i * LANES : (i + 1) * LANES
                ].astype(bf16)
            rot = part[:, LATENT:]
            dk_out[h, s, SLABS * chunk :, :] = (
                rot[: chunk // 2] + pltpu.roll(rot[chunk // 2 :], ROPE_DIM, 1)
            ).astype(bf16)
        return carry

    lax.fori_loop(0, keys.shape[1] * 2 * BLOCK // TILE, visit, 0)
    dq_own[...] = acc_own[...].astype(bf16)
    dq_peer[...] = acc_peer[...].astype(bf16)


def finish_kernel(ids, dq, dq_add, nope, key_up, dn_out, dr_out, keep, give):
    core = ids[1]
    for h in range(HEADS_HERE):
        cols = slice(h * NOPE_DIM, (h + 1) * NOPE_DIM)
        spot = slice(h * BLOCK, (h + 1) * BLOCK)
        both = [(dq[j, spot].astype(f32) + dq_add[j, spot].astype(f32)).astype(bf16) for j in range(2)]
        whole = jnp.concatenate(both, axis=0)
        grad = whole[:, :LATENT]
        dn_out[:, cols] = dot_nn(grad, key_up[:, cols]).astype(bf16)
        dr_out[:, h * ROPE_DIM : (h + 1) * ROPE_DIM] = whole[:, LATENT : LATENT + ROPE_DIM]
        mine, other = split_parity(dot_tn(grad, nope[:, cols]), keep.shape[0], core)
        slab = slice(h * mine.shape[1], (h + 1) * mine.shape[1])
        keep[:, slab, :] = mine
        give[:, slab, :] = other.astype(bf16)


def in_vmem(count):
    return [pl.BlockSpec(memory_space=pltpu.VMEM)] * count


def in_smem(count):
    return [pl.BlockSpec(memory_space=pltpu.SMEM)] * count


def shape(dims, dtype):
    return jax.ShapeDtypeStruct(dims, dtype)


IZ = ("inner", "z")
GRP = ("inner", "z", "core")


def to_partner(x):
    return lax.ppermute(x, "core", [(0, 1), (1, 0)])


def exchange(x, axis):
    return lax.all_to_all(x, axis, split_axis=0, concat_axis=0, tiled=True)


def to_all(x, axis):
    return exchange(jnp.broadcast_to(x, (lax.axis_size(axis), *x.shape)), axis)


def local(
    query_nope,
    query_rope,
    latent,
    key_rope,
    key_up,
    value_up,
    latent_out,
    out_grad,
    logsum,
    block_order,
):
    tokens = query_nope.shape[0]
    sets = lax.axis_size(IZ)
    heads = lax.axis_size("head")
    weight_rows = LATENT // (2 * sets)
    half = (sets, HEADS_HERE * weight_rows, LANES)
    params = pltpu.CompilerParams(vmem_limit_bytes=58 * 1024 * 1024)
    ids = jnp.stack([lax.axis_index(IZ), lax.axis_index("core")]).astype(jnp.int32)
    chunk = tokens // heads
    first = lax.axis_index("head") * chunk
    lat = lax.dynamic_slice_in_dim(latent, first, chunk, 0)
    rot = lax.dynamic_slice_in_dim(key_rope, first, chunk, 0)
    slabs = [lat[:, i * LANES : (i + 1) * LANES] for i in range(SLABS)]
    paired = jnp.concatenate([rot[: chunk // 2], rot[chunk // 2 :]], axis=1)
    mine = jnp.concatenate([*slabs, paired], axis=0)
    packed = mine.shape[0]
    keys = to_all(to_all(mine, IZ), "head")
    q, g, delta, value_keep, value_give = pl.pallas_call(
        prepare_kernel,
        in_specs=in_smem(1) + in_vmem(6),
        out_specs=in_vmem(5),
        out_shape=[
            shape((2, FLAT, WIDE), bf16),
            shape((2, FLAT, LATENT), bf16),
            shape((tokens, HEADS_HERE), f32),
            shape(half, f32),
            shape(half, bf16),
        ],
        compiler_params=params,
        name="prepare",
    )(ids, query_nope, query_rope, key_up, value_up, latent_out, out_grad)
    row_vals = jnp.stack([logsum, delta]).reshape(2, 2, BLOCK, HEADS_HERE)
    row_vals = row_vals.transpose(1, 0, 3, 2).reshape(2, 2, FLAT)
    q_peer, g_peer, vals_peer = to_partner(q), to_partner(g), to_partner(row_vals)
    value_part = (value_keep + to_partner(value_give).astype(f32)).astype(bf16)
    value_part, *_ = lax.optimization_barrier((value_part, keys, q_peer, g_peer, vals_peer))
    value_parts = exchange(value_part, IZ)
    attend = pl.pallas_call(
        attend_kernel,
        in_specs=in_smem(2) + in_vmem(7),
        out_specs=in_vmem(3),
        out_shape=[
            shape((heads, sets, packed, LANES), bf16),
            shape((2, FLAT, WIDE), bf16),
            shape((2, FLAT, WIDE), bf16),
        ],
        scratch_shapes=[
            pltpu.SMEM((block_order.shape[0],), jnp.int32),
            pltpu.SMEM((block_order.shape[0],), jnp.int32),
            pltpu.SMEM((block_order.shape[0],), jnp.int32),
            pltpu.VMEM((TILE, WIDE), f32),
            pltpu.VMEM((2, FLAT, WIDE), f32),
            pltpu.VMEM((2, FLAT, WIDE), f32),
        ],
        compiler_params=params,
        name="attend",
    )
    dk, dq, dq_give = attend(block_order, ids, keys, q, g, row_vals, q_peer, g_peer, vals_peer)
    dk, value_parts = lax.optimization_barrier((dk, value_parts))
    by_head = jnp.sum(exchange(dk, "head").astype(f32), axis=0).astype(bf16)
    dq_add = to_partner(dq_give)
    d_nope, d_rope, key_keep, key_give = pl.pallas_call(
        finish_kernel,
        in_specs=in_smem(1) + in_vmem(4),
        out_specs=in_vmem(4),
        out_shape=[
            shape(query_nope.shape, bf16),
            shape(query_rope.shape, bf16),
            shape(half, f32),
            shape(half, bf16),
        ],
        compiler_params=params,
        name="finish",
    )(ids, dq, dq_add, query_nope, key_up)
    key_part = (key_keep + to_partner(key_give).astype(f32)).astype(bf16)
    by_set = exchange(jnp.concatenate([by_head, key_part], axis=1), IZ)
    owned = jnp.sum(by_set[:, :packed].astype(f32), axis=0).astype(bf16)
    key_grad = jnp.sum(by_set[:, packed:].astype(f32), axis=0)
    value_grad = jnp.sum(value_parts.astype(f32), axis=0)
    total = to_all(owned, "head")
    d_lat = total[:, : SLABS * chunk].reshape(heads, SLABS, chunk, LANES)
    d_rot = total[:, SLABS * chunk :].reshape(heads, chunk // 2, 2, ROPE_DIM)

    def rows_of(grad):
        return grad.reshape(HEADS_HERE, weight_rows, LANES).transpose(1, 0, 2).reshape(
            weight_rows, HEADS_HERE * LANES
        )

    return (
        d_nope,
        d_rope,
        d_lat.transpose(0, 2, 1, 3).reshape(tokens, LATENT),
        d_rot.transpose(0, 2, 1, 3).reshape(tokens, ROPE_DIM),
        rows_of(key_grad),
        rows_of(value_grad),
    )


def solution(mesh):
    heads, inner, outer = mesh.devices.shape
    fine = Mesh(
        mesh.devices.reshape(heads, inner, outer // 2, 2), ("head", "inner", "z", "core")
    )
    rows = P(GRP, "head")
    return jax.shard_map(
        local,
        mesh=fine,
        in_specs=(rows, rows, P(GRP, None), P(GRP, None), P(None, "head"), P(None, "head"),
                  rows, rows, rows, P()),
        out_specs=(rows, rows, P(GRP, None), P(GRP, None), rows, rows),
        check_vma=False,
    )
```

```python
import jax
import jax.numpy as jnp
from jax import lax
from jax.experimental import pallas as pl
from jax.experimental.pallas import tpu as pltpu
from jax.sharding import Mesh, PartitionSpec as P

LATENT = 512
ROPE_DIM = 64
NOPE_DIM = 128
WIDE = 640
BLOCK = 64
HEADS_HERE = 8
FLAT = BLOCK * HEADS_HERE
TILE = 512
LANES = 128
SLABS = LATENT // LANES
PER_TILE = TILE // BLOCK
FACTOR = float(NOPE_DIM + ROPE_DIM) ** -0.5

f32 = jnp.float32
bf16 = jnp.bfloat16


def dot_nt(a, b):
    return lax.dot_general(a, b, (((1,), (1,)), ((), ())), preferred_element_type=f32)


def dot_nn(a, b):
    return lax.dot_general(a, b, (((1,), (0,)), ((), ())), preferred_element_type=f32)


def dot_tn(a, b):
    return lax.dot_general(a, b, (((0,), (0,)), ((), ())), preferred_element_type=f32)


def split_parity(rows, count, core):
    pieces = rows.reshape(count, 2, rows.shape[0] // (2 * count), rows.shape[1])
    even = pieces[:, 0]
    odd = pieces[:, 1]
    return jnp.where(core == 0, even, odd), jnp.where(core == 0, odd, even)


def prepare_kernel(
    ids, nope, rope, key_up, value_up, saved, upstream, q_out, g_out, delta_out, keep, give
):
    core = ids[1]
    zeros = jnp.zeros((2 * BLOCK, WIDE - LATENT - ROPE_DIM), bf16)
    for h in range(HEADS_HERE):
        cols = slice(h * NOPE_DIM, (h + 1) * NOPE_DIM)
        wide = slice(h * LATENT, (h + 1) * LATENT)
        query = dot_nt(nope[:, cols], key_up[:, cols]).astype(bf16)
        grad = dot_nt(upstream[:, cols], value_up[:, cols]).astype(bf16)
        kept = saved[:, wide]
        delta_out[:, h : h + 1] = jnp.sum(
            grad.astype(f32) * kept.astype(f32), axis=1, keepdims=True
        )
        mine, other = split_parity(dot_tn(kept, upstream[:, cols]), keep.shape[0], core)
        slab = slice(h * mine.shape[1], (h + 1) * mine.shape[1])
        keep[:, slab, :] = mine
        give[:, slab, :] = other.astype(bf16)
        tail = jnp.concatenate([rope[:, h * ROPE_DIM : (h + 1) * ROPE_DIM], zeros], axis=1)
        for j in range(2):
            rows = slice(j * BLOCK, (j + 1) * BLOCK)
            spot = slice(h * BLOCK, (h + 1) * BLOCK)
            q_out[j, spot, :LATENT] = query[rows]
            q_out[j, spot, LATENT:] = tail[rows]
            g_out[j, spot, :] = grad[rows]


def attend_kernel(
    order, ids, keys, q0, g0, v0, q1, g1, v1,
    dk_out, dq_own, dq_peer, where_at, place, seqs, dk_acc, acc_own, acc_peer,
):
    core = ids[1]
    blocks = order.shape[0]
    per_block = keys.shape[0] // 2
    chunk = BLOCK // per_block

    def note(i, carry):
        where_at[order[i]] = i
        return carry

    lax.fori_loop(0, blocks, note, 0)
    shard = ids[0] * 2
    seq_of = [order[2 * (shard + side) + j] for side in (core, 1 - core) for j in range(2)]

    def pick(s, carry):
        at = where_at[s]
        here = ((at // 2) % 2 == core).astype(jnp.int32)
        place[carry[0]] = (at // 4) * 2 + at % 2
        seqs[carry[0]] = s
        counts = [n + here * (s <= own).astype(jnp.int32) for n, own in zip(carry[1:], seq_of)]
        return (carry[0] + here, *counts)

    counts = lax.fori_loop(0, blocks, pick, (jnp.int32(0),) * 5)[1:]
    acc_own[...] = jnp.zeros(acc_own.shape, f32)
    acc_peer[...] = jnp.zeros(acc_peer.shape, f32)
    key_at = lax.broadcasted_iota(jnp.int32, (BLOCK, FLAT), 0)
    query_at = lax.broadcasted_iota(jnp.int32, (TILE, FLAT), 1) % BLOCK

    def unit(tile, key_pos, qj, gj, vj, acc, j, own):
        scores = dot_nt(tile, qj[j]) * FACTOR
        dprobs = dot_nt(tile[:, :LATENT], gj[j])
        visible = key_pos <= query_at + own * BLOCK
        probs = jnp.exp(jnp.where(visible, scores - vj[j, 0:1, :], -1e30))
        dscore = (probs * (dprobs - vj[j, 1:2, :]) * FACTOR).astype(bf16)
        low_probs = probs.astype(bf16)
        acc[j] += dot_tn(dscore, tile)
        grad = dot_nn(dscore, qj[j])
        dk_acc[:, :LATENT] += grad[:, :LATENT] + dot_nn(low_probs, gj[j])
        dk_acc[:, LATENT:] += grad[:, LATENT:]

    def unpack(h, s):
        slabs = [keys[h, s, i * chunk : (i + 1) * chunk, :] for i in range(SLABS)]
        rot = keys[h, s, SLABS * chunk :, :].astype(f32)
        both = jnp.concatenate([rot, pltpu.roll(rot, ROPE_DIM, 1)], axis=0).astype(bf16)
        return jnp.concatenate([*slabs, both], axis=1)

    def visit(t, carry):
        spots = [place[t * PER_TILE + i] for i in range(PER_TILE)]
        pieces = [
            ((k % 2) * per_block + piece, k // 2) for k in spots for piece in range(per_block)
        ]
        tile = jnp.concatenate([unpack(h, s) for h, s in pieces], axis=0)
        key_pos = jnp.concatenate(
            [key_at + seqs[t * PER_TILE + i] * BLOCK for i in range(PER_TILE)], axis=0
        )
        dk_acc[...] = jnp.zeros(dk_acc.shape, f32)
        sides = ((q0, g0, v0, acc_own), (q1, g1, v1, acc_peer))
        for n in range(4):
            @pl.when(t * PER_TILE < counts[n])
            def _():
                qj, gj, vj, acc = sides[n // 2]
                unit(tile, key_pos, qj, gj, vj, acc, n % 2, seq_of[n])
        for n, (h, s) in enumerate(pieces):
            part = dk_acc[n * chunk : (n + 1) * chunk]
            for i in range(SLABS):
                dk_out[h, s, i * chunk : (i + 1) * chunk, :] = part[
                    :, i * LANES : (i + 1) * LANES
                ].astype(bf16)
            rot = part[:, LATENT:]
            dk_out[h, s, SLABS * chunk :, :] = (
                rot[: chunk // 2] + pltpu.roll(rot[chunk // 2 :], ROPE_DIM, 1)
            ).astype(bf16)
        return carry

    lax.fori_loop(0, keys.shape[1] * 2 * BLOCK // TILE, visit, 0)
    dq_own[...] = acc_own[...].astype(bf16)
    dq_peer[...] = acc_peer[...].astype(bf16)


def finish_kernel(ids, dq, dq_add, nope, key_up, dn_out, dr_out, keep, give):
    core = ids[1]
    for h in range(HEADS_HERE):
        cols = slice(h * NOPE_DIM, (h + 1) * NOPE_DIM)
        spot = slice(h * BLOCK, (h + 1) * BLOCK)
        both = [(dq[j, spot].astype(f32) + dq_add[j, spot].astype(f32)).astype(bf16) for j in range(2)]
        whole = jnp.concatenate(both, axis=0)
        grad = whole[:, :LATENT]
        dn_out[:, cols] = dot_nn(grad, key_up[:, cols]).astype(bf16)
        dr_out[:, h * ROPE_DIM : (h + 1) * ROPE_DIM] = whole[:, LATENT : LATENT + ROPE_DIM]
        mine, other = split_parity(dot_tn(grad, nope[:, cols]), keep.shape[0], core)
        slab = slice(h * mine.shape[1], (h + 1) * mine.shape[1])
        keep[:, slab, :] = mine
        give[:, slab, :] = other.astype(bf16)


def in_vmem(count):
    return [pl.BlockSpec(memory_space=pltpu.VMEM)] * count


def in_smem(count):
    return [pl.BlockSpec(memory_space=pltpu.SMEM)] * count


def shape(dims, dtype):
    return jax.ShapeDtypeStruct(dims, dtype)


IZ = ("inner", "z")
GRP = ("inner", "z", "core")


def to_partner(x):
    return lax.ppermute(x, "core", [(0, 1), (1, 0)])


def exchange(x, axis):
    return lax.all_to_all(x, axis, split_axis=0, concat_axis=0, tiled=True)


def halved(parts):
    bits = lax.axis_size("z").bit_length() - 1
    left = parts.reshape((2,) * (1 + bits) + parts.shape[1:])
    z = lax.axis_index("z")
    for step in range(1 + bits):
        axis, flip = ("inner", 1) if step == 0 else ("z", 1 << (step - 1))
        bit = lax.axis_index("inner") if step == 0 else (z // flip) % 2
        dim = 0 if step == 0 else bits - step
        kept = lax.dynamic_index_in_dim(left, bit, dim, keepdims=False)
        given = lax.dynamic_index_in_dim(left, 1 - bit, dim, keepdims=False)
        pairs = [(i, i ^ flip) for i in range(lax.axis_size(axis))]
        left = kept.astype(f32) + lax.ppermute(given, axis, pairs).astype(f32)
        left = left.astype(bf16) if step < bits else left
    return left


def to_all(x, axis):
    return exchange(jnp.broadcast_to(x, (lax.axis_size(axis), *x.shape)), axis)


def whole(
    query_nope,
    query_rope,
    latent,
    key_rope,
    key_up,
    value_up,
    latent_out,
    out_grad,
    logsum,
    block_order,
):
    tokens = query_nope.shape[0]
    sets = lax.axis_size(IZ)
    heads = lax.axis_size("head")
    weight_rows = LATENT // (2 * sets)
    half = (sets, HEADS_HERE * weight_rows, LANES)
    params = pltpu.CompilerParams(vmem_limit_bytes=58 * 1024 * 1024)
    ids = jnp.stack([lax.axis_index(IZ), lax.axis_index("core")]).astype(jnp.int32)
    chunk = tokens // heads
    first = lax.axis_index("head") * chunk
    lat = lax.dynamic_slice_in_dim(latent, first, chunk, 0)
    rot = lax.dynamic_slice_in_dim(key_rope, first, chunk, 0)
    slabs = [lat[:, i * LANES : (i + 1) * LANES] for i in range(SLABS)]
    paired = jnp.concatenate([rot[: chunk // 2], rot[chunk // 2 :]], axis=1)
    mine = jnp.concatenate([*slabs, paired], axis=0)
    packed = mine.shape[0]
    keys = to_all(to_all(mine, IZ), "head")
    q, g, delta, value_keep, value_give = pl.pallas_call(
        prepare_kernel,
        in_specs=in_smem(1) + in_vmem(6),
        out_specs=in_vmem(5),
        out_shape=[
            shape((2, FLAT, WIDE), bf16),
            shape((2, FLAT, LATENT), bf16),
            shape((tokens, HEADS_HERE), f32),
            shape(half, f32),
            shape(half, bf16),
        ],
        compiler_params=params,
        name="prepare",
    )(ids, query_nope, query_rope, key_up, value_up, latent_out, out_grad)
    row_vals = jnp.stack([logsum, delta]).reshape(2, 2, BLOCK, HEADS_HERE)
    row_vals = row_vals.transpose(1, 0, 3, 2).reshape(2, 2, FLAT)
    q_peer, g_peer, vals_peer = to_partner(q), to_partner(g), to_partner(row_vals)
    value_part = (value_keep + to_partner(value_give).astype(f32)).astype(bf16)
    value_part, *_ = lax.optimization_barrier((value_part, keys, q_peer, g_peer, vals_peer))
    value_parts = exchange(value_part, IZ)
    attend = pl.pallas_call(
        attend_kernel,
        in_specs=in_smem(2) + in_vmem(7),
        out_specs=in_vmem(3),
        out_shape=[
            shape((heads, sets, packed, LANES), bf16),
            shape((2, FLAT, WIDE), bf16),
            shape((2, FLAT, WIDE), bf16),
        ],
        scratch_shapes=[
            pltpu.SMEM((block_order.shape[0],), jnp.int32),
            pltpu.SMEM((block_order.shape[0],), jnp.int32),
            pltpu.SMEM((block_order.shape[0],), jnp.int32),
            pltpu.VMEM((TILE, WIDE), f32),
            pltpu.VMEM((2, FLAT, WIDE), f32),
            pltpu.VMEM((2, FLAT, WIDE), f32),
        ],
        compiler_params=params,
        name="attend",
    )
    dk, dq, dq_give = attend(
        block_order, ids, keys, q, g, row_vals, q_peer, g_peer, vals_peer
    )
    dk, value_parts = lax.optimization_barrier((dk, value_parts))
    from_heads = exchange(dk, "head")
    by_head = jnp.sum(from_heads.astype(f32), axis=0).astype(bf16)
    dq_add = to_partner(dq_give)
    finish = pl.pallas_call(
        finish_kernel,
        in_specs=in_smem(1) + in_vmem(4),
        out_specs=in_vmem(4),
        out_shape=[
            shape(query_nope.shape, bf16),
            shape(query_rope.shape, bf16),
            shape(half, f32),
            shape(half, bf16),
        ],
        compiler_params=params,
        name="finish",
    )
    d_nope, d_rope, key_keep, key_give = finish(ids, dq, dq_add, query_nope, key_up)
    key_part = (key_keep + to_partner(key_give).astype(f32)).astype(bf16)
    key_grad = halved(key_part)
    owned = jnp.sum(exchange(by_head, IZ).astype(f32), axis=0).astype(bf16)
    value_grad = jnp.sum(value_parts.astype(f32), axis=0)
    total = to_all(owned, "head")
    d_lat = total[:, : SLABS * chunk].reshape(heads, SLABS, chunk, LANES)
    d_rot = total[:, SLABS * chunk :].reshape(heads, chunk // 2, 2, ROPE_DIM)

    def rows_of(grad):
        return grad.reshape(HEADS_HERE, weight_rows, LANES).transpose(1, 0, 2).reshape(
            weight_rows, HEADS_HERE * LANES
        )

    return (
        d_nope,
        d_rope,
        d_lat.transpose(0, 2, 1, 3).reshape(tokens, LATENT),
        d_rot.transpose(0, 2, 1, 3).reshape(tokens, ROPE_DIM),
        rows_of(key_grad),
        rows_of(value_grad),
    )


def solution(mesh):
    heads, inner, outer = mesh.devices.shape
    fine = Mesh(
        mesh.devices.reshape(heads, inner, outer // 2, 2), ("head", "inner", "z", "core")
    )
    rows = P(GRP, "head")
    return jax.shard_map(
        whole,
        mesh=fine,
        in_specs=(rows, rows, P(GRP, None), P(GRP, None), P(None, "head"), P(None, "head"),
                  rows, rows, rows, P()),
        out_specs=(rows, rows, P(GRP, None), P(GRP, None), rows, rows),
        check_vma=False,
    )
```
